512 devices in a mesh: seq: 16 (over y, z_lo), outer: 32 (over z_hi, x, core).
Axes of the slice: x: 4, y: 4, z: 16 (z_hi: 4, z_lo: 4; z = z_hi * 4 + z_lo), core: 2. Of those that a mesh axis runs over, the one named last changes fastest.
Arguments:
- queries: bfloat16 [262144, 2048], P(('outer', 'seq')), may hold values from -41 to 41
- keys: bfloat16 [262144, 512], P(('outer', 'seq')), may hold values from -6 to 6
- values: bfloat16 [262144, 512], P(('outer', 'seq')), may hold values from -6 to 6
Outputs:
- attended: bfloat16 [262144, 2048], P(('outer', 'seq'))
The draws below stay inside these ranges and needn't reach their ends.
All inputs are finite; a program needn't handle non-finite values.
Results may differ from the reference program's by a relative error of at most 0.014.
Values may be sent and summed in bfloat16 or wider, within the bound.
No kernel may reach another device: no remote copies, remote signals or barrier semaphores. Data moves between devices by JAX's collectives and lax.ppermute only.
A program may use at most 64 MiB of HBM per device.

```python
import jax
import jax.numpy as jnp
from jax import lax

HD = 128
QHEADS = 16
KVHEADS = 4
BLOCK = 128
POOL = 8
TOKENS = 262144


def draw_shared_keys(key):
    source = jax.random.fold_in(key, 101)
    return jax.random.truncated_normal(source, -6.0, 6.0, (TOKENS, KVHEADS * HD), jnp.float32)


def draw_keys(key, part):
    return draw_shared_keys(key).astype(jnp.bfloat16)


def draw_queries(key, part):
    drawn_draw = jax.random.truncated_normal(jax.random.fold_in(key, 202), -6.0, 6.0, (TOKENS, QHEADS * HD), jnp.float32)
    return drawn_draw.astype(jnp.bfloat16)


def level_of(key, dims, cuts, least, largest):
    def one(dim, blocks):
        heights = jax.random.uniform(jax.random.fold_in(jax.random.fold_in(key, 6), dim), (blocks,), jnp.float32, least / len(cuts), largest / len(cuts))
        return jnp.repeat(jnp.exp(heights), dims[dim] // blocks).reshape((-1,) + (1,) * (len(dims) - dim - 1))

    factor_of = one(*cuts[0])
    for cut in cuts[1:]:
        factor_of = factor_of * one(*cut)
    return factor_of


def centred(key, shape, width, limit, shards=(), kind=jnp.bfloat16):
    values = jax.random.normal(key, shape, jnp.float32) * width
    if len(shards) > 0:
        values = level_of(key, shape, shards, -0.22, 0.18) * values
    return jnp.clip(values, min=-limit, max=limit).astype(kind)


def setup_inputs(seed: int = 0) -> dict:
    arg_keys = jax.random.split(jax.random.key(seed), 4)
    queries = draw_queries(jax.random.fold_in(arg_keys[3], 71), 0)
    keys = draw_keys(jax.random.fold_in(arg_keys[3], 71), 0)
    values = centred(arg_keys[2], (TOKENS, KVHEADS * HD), 1.0, 6.0, ((0, 512),))
    return dict(queries=queries, keys=keys, values=values)


def pool_level(element_item):
    span_length = element_item.shape[0]
    summed = element_item.astype(jnp.float32).reshape(span_length // POOL, POOL, element_item.shape[1]).sum(axis=1)
    return lax.optimization_barrier((summed * (POOL ** -0.5)).astype(jnp.bfloat16))


def attend_block(query_rows, key_set, value_set, valid):
    group_size = QHEADS // KVHEADS
    head_queries = query_rows.reshape(BLOCK, KVHEADS, group_size, HD).transpose(1, 0, 2, 3)
    head_keys = key_set.reshape(-1, KVHEADS, HD).transpose(1, 0, 2)
    head_values = value_set.reshape(-1, KVHEADS, HD).transpose(1, 0, 2)

    def one_head(operands):
        part_q, part_k, part_v = operands
        scores = jnp.einsum("tgd,sd->gts", part_q.astype(jnp.float32), part_k.astype(jnp.float32)) * (HD ** -0.5)
        scores = jnp.where(valid, scores, -jnp.inf)
        highest = jnp.max(scores, axis=2, keepdims=True)
        weights = jnp.exp(scores - highest)
        totals = jnp.sum(weights, axis=2)
        rounded = lax.optimization_barrier(weights.astype(jnp.bfloat16))
        mixed = jnp.einsum("gts,sd->tgd", rounded.astype(jnp.float32), part_v.astype(jnp.float32))
        return (mixed / totals.T[:, :, None]).astype(jnp.bfloat16)

    outputs = lax.map(one_head, (head_queries, head_keys, head_values))
    return outputs.transpose(1, 0, 2, 3).reshape(BLOCK, QHEADS * HD)


def reference(queries, keys, values):
    levels = [(keys, values)]
    for level_index in range(3):
        levels.append((pool_level(levels[-1][0]), pool_level(levels[-1][1])))
    padded = [(jnp.pad(pair[0], ((BLOCK, 2 * BLOCK), (0, 0))), jnp.pad(pair[1], ((BLOCK, 2 * BLOCK), (0, 0)))) for pair in levels[:3]]
    blocks = queries.shape[0] // BLOCK
    top_rows = levels[3][0].shape[0]

    def one_block(fine_index):
        key_parts = []
        value_parts = []
        mask_parts = []
        for level_index in range(3):
            coarse = fine_index // (POOL ** level_index)
            start_row = (coarse * BLOCK).astype(jnp.int32)
            key_parts.append(lax.dynamic_slice_in_dim(padded[level_index][0], start_row, 3 * BLOCK, 0))
            value_parts.append(lax.dynamic_slice_in_dim(padded[level_index][1], start_row, 3 * BLOCK, 0))
            positions = (coarse - 1) * BLOCK + jnp.arange(3 * BLOCK, dtype=jnp.int32)
            mask_parts.append((positions >= 0) & (positions < levels[level_index][0].shape[0]))
        key_parts.append(levels[3][0])
        value_parts.append(levels[3][1])
        mask_parts.append(jnp.ones((top_rows,), dtype=bool))
        query_rows = lax.dynamic_slice_in_dim(queries, (fine_index * BLOCK).astype(jnp.int32), BLOCK, 0)
        return attend_block(query_rows, jnp.concatenate(key_parts, axis=0), jnp.concatenate(value_parts, axis=0), jnp.concatenate(mask_parts, axis=0))

    result = lax.map(one_block, jnp.arange(blocks, dtype=jnp.int32))
    return result.reshape(queries.shape[0], QHEADS * HD)
```

```python
import functools

import jax
import jax.numpy as jnp
from jax import lax
from jax.experimental import pallas as pl
from jax.experimental.pallas import tpu as pltpu
from jax.sharding import Mesh
from jax.sharding import PartitionSpec as P


HD = 128
QHEADS = 16
KVHEADS = 4
GROUP = QHEADS // KVHEADS
BLOCK = 128
POOL = 8
WIDTH = KVHEADS * HD
TILE = 256
SCALE = HD ** (-0.5) * 1.4426950408889634
FINE = ("y", "z_lo", "z_hi", "x", "core")
TOKEN_ORDER = ("z_hi", "x", "core", "y", "z_lo")
SEQ, OUTER = 16, 32
VMEM = 67043328
COUNT = SEQ * OUTER


def holds(flags, bit):
    return (flags[0] >> bit) % 2 == 1


def pooling_matrix(rows):
    first = lax.broadcasted_iota(jnp.int32, (rows // POOL, rows), 0)
    second = lax.broadcasted_iota(jnp.int32, (rows // POOL, rows), 1)
    return jnp.where(second // POOL == first, 1.0, 0.0).astype(jnp.bfloat16)


def pooled(rows):
    summed = jnp.dot(pooling_matrix(rows.shape[0]), rows, preferred_element_type=jnp.float32)
    return (summed * POOL ** (-0.5)).astype(jnp.bfloat16)


def pool_kernel(flags, k_ref, v_ref, first_ref, second_ref, partner_ref, other_ref):
    rows = k_ref.shape[0]
    odd = holds(flags, 5)
    for part, ref in enumerate((k_ref, v_ref)):
        columns = slice(part * WIDTH, (part + 1) * WIDTH)
        one = pooled(ref[...])
        first_ref[:, columns] = one
        partner_ref[BLOCK:, columns] = one
        other_ref[BLOCK:, columns] = one
        two = pooled(one)
        for copy in range(second_ref.shape[0]):
            second_ref[copy, :, columns] = two

        @pl.when(odd)
        def _():
            partner_ref[:BLOCK, columns] = ref[:BLOCK]
            other_ref[:BLOCK, columns] = ref[rows - BLOCK :]

        @pl.when(jnp.logical_not(odd))
        def _():
            partner_ref[:BLOCK, columns] = ref[rows - BLOCK :]
            other_ref[:BLOCK, columns] = ref[:BLOCK]


def pool_local(flags, keys, values):
    first = keys.shape[0] // POOL
    shapes = [(first,), (SEQ, first // POOL), (BLOCK + first,), (BLOCK + first,)]
    vmem = pl.BlockSpec(memory_space=pltpu.VMEM)
    return pl.pallas_call(
        pool_kernel,
        in_specs=[pl.BlockSpec(memory_space=pltpu.SMEM), vmem, vmem],
        out_shape=[jax.ShapeDtypeStruct((*n, 2 * WIDTH), jnp.bfloat16) for n in shapes],
        compiler_params=pltpu.CompilerParams(vmem_limit_bytes=VMEM),
        name="pool_local",
    )(flags, keys, values)


def pool_again_kernel(rows_ref, out_ref):
    rows = pooled(rows_ref[...])
    for copy in range(out_ref.shape[0]):
        out_ref[copy] = rows


def pool_again(rows, copies):
    return pl.pallas_call(
        pool_again_kernel,
        out_shape=jax.ShapeDtypeStruct((copies, rows.shape[0] // POOL, rows.shape[1]), jnp.bfloat16),
        compiler_params=pltpu.CompilerParams(vmem_limit_bytes=VMEM),
        name="pool_again",
    )(rows)


def chunks_of(windows):
    tiles, tile, room = [], [], TILE
    for start, length in windows:
        while length:
            take = min(room, length)
            tile.append((start, take))
            start, length, room = start + take, length - take, room - take
            if room == 0:
                tiles.append(tile)
                tile, room = [], TILE
    if tile:
        tiles.append(tile)
    return tiles


def rows_of(ref, tile):
    parts = [ref[start : start + length, :] for start, length in tile]
    return parts[0] if len(parts) == 1 else jnp.concatenate(parts, axis=0)


def attend_kernel(count, pieces, swaps, guards, windows, earlier, later, *refs):
    refs = list(refs)
    flags = refs.pop(0)
    q_ref = refs.pop(0)
    sources = [(refs.pop(0), refs.pop(0)) for _ in range(count)]
    before = (refs.pop(0), refs.pop(0)) if earlier else None
    o_ref = refs.pop(0)
    lse_ref = refs.pop(0) if later else None
    kx, vx, s_ref, p_ref, m_ref = refs
    places, held = [], 0
    for _, _, rows in pieces:
        places.append(held)
        held += rows

    def fill(piece, taken):
        source, first, rows = pieces[taken]
        here = slice(places[piece], places[piece] + rows)
        kx[here, :] = sources[source][0][first : first + rows, :]
        vx[here, :HD] = sources[source][1][first : first + rows, :]

    vx[:, HD:] = jnp.ones((held, HD), jnp.bfloat16)
    for piece in range(len(pieces)):
        if piece not in swaps:
            fill(piece, piece)
    for order, wanted in ((swaps, False), (swaps[::-1], True)) if swaps else ():

        @pl.when(holds(flags, 5) == wanted)
        def _():
            for piece, taken in zip(swaps, order):
                fill(piece, taken)

    for piece, (flag, stand_in) in guards.items():
        rows = pieces[piece][2]
        here = slice(places[piece], places[piece] + rows)

        @pl.when(jnp.logical_not(holds(flags, flag)))
        def _():
            kx[here, :] = kx[places[stand_in] : places[stand_in] + rows, :]
            vx[here, :] = jnp.zeros((rows, 2 * HD), jnp.bfloat16)

    blocks = q_ref.shape[0] // BLOCK
    rows = GROUP * BLOCK
    step = 32

    def score(b):
        slot = b % 2
        q4 = jnp.concatenate(
            [q_ref[b * BLOCK : (b + 1) * BLOCK, g * HD : (g + 1) * HD] for g in range(GROUP)], axis=0
        )
        at = 0
        for tile in chunks_of(windows(b)):
            part = rows_of(kx, tile)
            s_ref[slot, :, at : at + part.shape[0]] = lax.dot_general(
                q4, part, (((1,), (1,)), ((), ())), preferred_element_type=jnp.float32
            )
            at += part.shape[0]
        for r in range(0, rows, step):
            here = slice(r, r + step)
            top = jnp.max(s_ref[slot, here, :], axis=1, keepdims=True) * SCALE
            top = jnp.broadcast_to(top, (step, HD))
            if earlier:
                top = jnp.maximum(top, before[1][b * rows + r : b * rows + r + step, :])
            m_ref[slot, here, :] = top

    def finish(b):
        slot = b % 2
        width = s_ref.shape[2]
        for r in range(0, rows, step):
            here = slice(r, r + step)
            top = m_ref[slot, here, :]
            for a in range(0, width, HD):
                weight = jnp.exp2(s_ref[slot, here, a : a + HD] * SCALE - top)
                p_ref[slot, here, a : a + HD] = weight.astype(jnp.bfloat16)
        total = None
        at = 0
        for tile in chunks_of(windows(b)):
            part = rows_of(vx, tile)
            mixed = jnp.dot(
                p_ref[slot, :, at : at + part.shape[0]], part, preferred_element_type=jnp.float32
            )
            total = mixed if total is None else total + mixed
            at += part.shape[0]
        for g in range(GROUP):
            head = slice(g * BLOCK, (g + 1) * BLOCK)
            tokens = slice(b * BLOCK, (b + 1) * BLOCK)
            columns = slice(g * HD, (g + 1) * HD)
            upper, lower = total[head, :HD], total[head, HD:]
            if earlier:
                place = slice(b * rows + g * BLOCK, b * rows + (g + 1) * BLOCK)
                share = jnp.exp2(before[1][place, :] - m_ref[slot, head, :])
                upper = upper + share * before[0][tokens, columns].astype(jnp.float32)
                lower = lower + share
            o_ref[tokens, columns] = (upper / lower).astype(o_ref.dtype)
            if later:
                place = slice(b * rows + g * BLOCK, b * rows + (g + 1) * BLOCK)
                lse_ref[place, :] = m_ref[slot, head, :] + jnp.log2(lower)

    score(0)
    for b in range(blocks):
        if b + 1 < blocks:
            score(b + 1)
        finish(b)


def attend(flags, queries, sources, pieces, swaps, guards, windows, width, before=None, later=False):
    tokens = queries.shape[0]
    rows = tokens * GROUP
    held = sum(n for _, _, n in pieces)
    wide = pl.BlockSpec((tokens, GROUP * HD), lambda h: (0, h))
    tall = pl.BlockSpec((rows, HD), lambda h: (h, 0))

    def narrow(array, offset):
        return pl.BlockSpec((array.shape[0], HD), lambda h: (0, h + offset))

    in_specs = [pl.BlockSpec(memory_space=pltpu.SMEM), wide]
    operands = [flags, queries]
    for k, k_at, v, v_at in sources:
        in_specs += [narrow(k, k_at), narrow(v, v_at)]
        operands += [k, v]
    if before is not None:
        in_specs += [wide, tall]
        operands += list(before)
    out_shape = [jax.ShapeDtypeStruct(queries.shape, jnp.bfloat16)]
    out_specs = [wide]
    if later:
        out_shape.append(jax.ShapeDtypeStruct((KVHEADS * rows, HD), jnp.float32))
        out_specs.append(tall)
    unit = GROUP * BLOCK
    return pl.pallas_call(
        functools.partial(
            attend_kernel, len(sources), pieces, swaps, guards, windows, before is not None, later
        ),
        grid=(KVHEADS,),
        in_specs=in_specs,
        out_specs=out_specs,
        out_shape=out_shape,
        scratch_shapes=[
            pltpu.VMEM((held, HD), jnp.bfloat16),
            pltpu.VMEM((held, 2 * HD), jnp.bfloat16),
            pltpu.VMEM((2, unit, width), jnp.float32),
            pltpu.VMEM((2, unit, width), jnp.bfloat16),
            pltpu.VMEM((2, unit, HD), jnp.float32),
        ],
        compiler_params=pltpu.CompilerParams(
            dimension_semantics=("arbitrary",), vmem_limit_bytes=VMEM
        ),
        cost_estimate=pl.CostEstimate(
            flops=4 * tokens * QHEADS * HD * width,
            bytes_accessed=6 * tokens * QHEADS * HD,
            transcendentals=tokens * QHEADS * width,
        ),
    )(*operands)


def placed_at(token_index):
    return (token_index % SEQ) * OUTER + token_index // SEQ


def moved(rows, source_of):
    route = [
        (placed_at(source_of(i)), placed_at(i)) for i in range(COUNT) if 0 <= source_of(i) < COUNT
    ]
    return lax.ppermute(rows, FINE, route)


def exchanged(copies, axis):
    result = lax.all_to_all(copies, axis, 0, 0, tiled=True)
    return result.reshape(-1, result.shape[-1])


def one_device(queries, keys, values):
    outer = (lax.axis_index("z_hi") * 4 + lax.axis_index("x")) * 2 + lax.axis_index("core")
    index = outer * SEQ + lax.axis_index("y") * 4 + lax.axis_index("z_lo")
    flags = [
        index > 0,
        index < COUNT - 1,
        (index >= 2) & (index < COUNT - 2),
        (outer > 0) & (outer < OUTER - 1),
        (index > 0) & (index < COUNT - 1),
        index % 2,
        (index != 1) & (index != COUNT - 2),
    ]
    flags = sum(jnp.asarray(e, jnp.int32) << k for k, e in enumerate(flags)).reshape(1)

    first, second, to_partner, to_other = pool_local(flags, keys, values)

    group = exchanged(second, ("y", "z_lo"))
    partner = moved(to_partner, lambda i: i ^ 1)
    other = moved(to_other, lambda i: i + 1 if i % 2 else i - 1)
    two = moved(first, lambda i: i ^ 2)
    third = moved(first, lambda i: i - 3 if i % 2 else i + 3)
    far = moved(first, lambda i: i - 2 if i % 4 < 2 else i + 2)

    top = exchanged(pool_again(group, 4), "z_hi")
    top = exchanged(jnp.broadcast_to(top[None], (4, *top.shape)), "x")
    group_pair = moved(group, lambda i: i ^ SEQ)
    group_other = moved(group, lambda i: i + SEQ if (i // SEQ) % 2 else i - SEQ)
    top_pair = moved(top, lambda i: i ^ SEQ)

    def both(array):
        return (array, 0, array, KVHEADS)

    def whole(arrays):
        return [(k, 0, array[0].shape[0]) for k, array in enumerate(arrays)]

    rows = keys.shape[0]
    firsts = first.shape[0]
    near = [(keys, 0, values, 0)] + [both(a) for a in (other, partner, first, two, third, far)]
    pieces = [(1, 0, BLOCK), (0, 0, rows), (2, 0, BLOCK), (3, 0, firsts), (2, BLOCK, firsts)]
    pieces += [(1, BLOCK, firsts), (4, 0, firsts), (5, 0, firsts), (6, 0, firsts)]
    part, lse = attend(
        flags,
        queries,
        near,
        pieces,
        [0, 2],
        {0: (0, 1), 2: (1, 1), 5: (4, 3), 7: (6, 3), 8: (2, 3)},
        lambda b: [(b * BLOCK, 3 * BLOCK), (rows + 2 * BLOCK, 3 * BLOCK)],
        6 * BLOCK,
        later=True,
    )
    coarse = [both(a) for a in (top, top_pair, group, group_pair, group_other)]
    tops = 2 * top.shape[0]
    (out,) = attend(
        flags,
        queries,
        coarse,
        whole(coarse),
        [],
        {4: (3, 2)},
        lambda b: [(0, tops + 3 * BLOCK)],
        tops + 3 * BLOCK,
        before=(part, lse),
    )
    return out


def solution(mesh):
    assert mesh.axis_names == ("seq", "outer")
    split = Mesh(mesh.devices.reshape(4, 4, 4, 4, 2), FINE)
    placed = P(TOKEN_ORDER, None)
    return jax.shard_map(
        one_device, mesh=split, in_specs=(placed,) * 3, out_specs=placed, check_vma=False
    )
```

```python
import functools

import jax
import jax.numpy as jnp
from jax import lax
from jax.experimental import pallas as pl
from jax.experimental.pallas import tpu as pltpu
from jax.sharding import Mesh
from jax.sharding import PartitionSpec as P


HD = 128
QHEADS = 16
KVHEADS = 4
GROUP = QHEADS // KVHEADS
BLOCK = 128
POOL = 8
WIDTH = KVHEADS * HD
TILE = 256
SCALE = HD ** (-0.5) * 1.4426950408889634
FINE = ("y", "z_lo", "z_hi", "x", "core")
TOKEN_ORDER = ("z_hi", "x", "core", "y", "z_lo")
SEQ, OUTER = 16, 32
VMEM = 67043328
COUNT = SEQ * OUTER


def holds(flags, bit):
    return (flags[0] >> bit) % 2 == 1


def pooling_matrix(rows):
    first = lax.broadcasted_iota(jnp.int32, (rows // POOL, rows), 0)
    second = lax.broadcasted_iota(jnp.int32, (rows // POOL, rows), 1)
    return jnp.where(second // POOL == first, 1.0, 0.0).astype(jnp.bfloat16)


def pooled(rows):
    summed = jnp.dot(pooling_matrix(rows.shape[0]), rows, preferred_element_type=jnp.float32)
    return (summed * POOL ** (-0.5)).astype(jnp.bfloat16)


def pool_kernel(flags, k_ref, v_ref, first_ref, second_ref, partner_ref, other_ref):
    rows = k_ref.shape[0]
    odd = holds(flags, 5)
    for part, ref in enumerate((k_ref, v_ref)):
        columns = slice(part * WIDTH, (part + 1) * WIDTH)
        one = pooled(ref[...])
        first_ref[:, columns] = one
        partner_ref[BLOCK:, columns] = one
        other_ref[BLOCK:, columns] = one
        two = pooled(one)
        for copy in range(second_ref.shape[0]):
            second_ref[copy, :, columns] = two

        @pl.when(odd)
        def _():
            partner_ref[:BLOCK, columns] = ref[:BLOCK]
            other_ref[:BLOCK, columns] = ref[rows - BLOCK :]

        @pl.when(jnp.logical_not(odd))
        def _():
            partner_ref[:BLOCK, columns] = ref[rows - BLOCK :]
            other_ref[:BLOCK, columns] = ref[:BLOCK]


def pool_local(flags, keys, values):
    first = keys.shape[0] // POOL
    shapes = [(first,), (SEQ, first // POOL), (BLOCK + first,), (BLOCK + first,)]
    vmem = pl.BlockSpec(memory_space=pltpu.VMEM)
    return pl.pallas_call(
        pool_kernel,
        in_specs=[pl.BlockSpec(memory_space=pltpu.SMEM), vmem, vmem],
        out_shape=[jax.ShapeDtypeStruct((*n, 2 * WIDTH), jnp.bfloat16) for n in shapes],
        compiler_params=pltpu.CompilerParams(vmem_limit_bytes=VMEM),
        name="pool_local",
    )(flags, keys, values)


def pool_again_kernel(rows_ref, out_ref):
    rows = pooled(rows_ref[...])
    for copy in range(out_ref.shape[0]):
        out_ref[copy] = rows


def pool_again(rows, copies):
    return pl.pallas_call(
        pool_again_kernel,
        out_shape=jax.ShapeDtypeStruct((copies, rows.shape[0] // POOL, rows.shape[1]), jnp.bfloat16),
        compiler_params=pltpu.CompilerParams(vmem_limit_bytes=VMEM),
        name="pool_again",
    )(rows)


def chunks_of(windows):
    tiles, tile, room = [], [], TILE
    for start, length in windows:
        while length:
            take = min(room, length)
            tile.append((start, take))
            start, length, room = start + take, length - take, room - take
            if room == 0:
                tiles.append(tile)
                tile, room = [], TILE
    if tile:
        tiles.append(tile)
    return tiles


def rows_of(ref, tile):
    parts = [ref[start : start + length, :] for start, length in tile]
    return parts[0] if len(parts) == 1 else jnp.concatenate(parts, axis=0)


def attend_kernel(count, pieces, swaps, guards, windows, earlier, later, *refs):
    refs = list(refs)
    flags = refs.pop(0)
    q_ref = refs.pop(0)
    sources = [(refs.pop(0), refs.pop(0)) for _ in range(count)]
    before = (refs.pop(0), refs.pop(0)) if earlier else None
    o_ref = refs.pop(0)
    lse_ref = refs.pop(0) if later else None
    kx, vx, s_ref, p_ref, m_ref = refs
    places, held = [], 0
    for _, _, rows in pieces:
        places.append(held)
        held += rows

    def fill(piece, taken):
        source, first, rows = pieces[taken]
        here = slice(places[piece], places[piece] + rows)
        kx[here, :] = sources[source][0][first : first + rows, :]
        vx[here, :HD] = sources[source][1][first : first + rows, :]

    vx[:, HD:] = jnp.ones((held, HD), jnp.bfloat16)
    for piece in range(len(pieces)):
        if piece not in swaps:
            fill(piece, piece)
    for order, wanted in ((swaps, False), (swaps[::-1], True)) if swaps else ():

        @pl.when(holds(flags, 5) == wanted)
        def _():
            for piece, taken in zip(swaps, order):
                fill(piece, taken)

    for piece, (flag, stand_in) in guards.items():
        rows = pieces[piece][2]
        here = slice(places[piece], places[piece] + rows)

        @pl.when(jnp.logical_not(holds(flags, flag)))
        def _():
            kx[here, :] = kx[places[stand_in] : places[stand_in] + rows, :]
            vx[here, :] = jnp.zeros((rows, 2 * HD), jnp.bfloat16)

    blocks = q_ref.shape[0] // BLOCK
    rows = GROUP * BLOCK
    step = 32

    def score(b):
        slot = b % 2
        q4 = jnp.concatenate(
            [q_ref[b * BLOCK : (b + 1) * BLOCK, g * HD : (g + 1) * HD] for g in range(GROUP)], axis=0
        )
        at = 0
        for tile in chunks_of(windows(b)):
            part = rows_of(kx, tile)
            s_ref[slot, :, at : at + part.shape[0]] = lax.dot_general(
                q4, part, (((1,), (1,)), ((), ())), preferred_element_type=jnp.float32
            )
            at += part.shape[0]
        for r in range(0, rows, step):
            here = slice(r, r + step)
            top = jnp.max(s_ref[slot, here, :], axis=1, keepdims=True) * SCALE
            top = jnp.broadcast_to(top, (step, HD))
            if earlier:
                top = jnp.maximum(top, before[1][b * rows + r : b * rows + r + step, :])
            m_ref[slot, here, :] = top

    def finish(b):
        slot = b % 2
        width = s_ref.shape[2]
        for r in range(0, rows, step):
            here = slice(r, r + step)
            top = m_ref[slot, here, :]
            for a in range(0, width, HD):
                weight = jnp.exp2(s_ref[slot, here, a : a + HD] * SCALE - top)
                p_ref[slot, here, a : a + HD] = weight.astype(jnp.bfloat16)
        total = None
        at = 0
        for tile in chunks_of(windows(b)):
            part = rows_of(vx, tile)
            mixed = jnp.dot(
                p_ref[slot, :, at : at + part.shape[0]], part, preferred_element_type=jnp.float32
            )
            total = mixed if total is None else total + mixed
            at += part.shape[0]
        for g in range(GROUP):
            head = slice(g * BLOCK, (g + 1) * BLOCK)
            tokens = slice(b * BLOCK, (b + 1) * BLOCK)
            columns = slice(g * HD, (g + 1) * HD)
            upper, lower = total[head, :HD], total[head, HD:]
            if earlier:
                place = slice(b * rows + g * BLOCK, b * rows + (g + 1) * BLOCK)
                share = jnp.exp2(before[1][place, :] - m_ref[slot, head, :])
                upper = upper + share * before[0][tokens, columns].astype(jnp.float32)
                lower = lower + share
            o_ref[tokens, columns] = (upper / lower).astype(o_ref.dtype)
            if later:
                place = slice(b * rows + g * BLOCK, b * rows + (g + 1) * BLOCK)
                lse_ref[place, :] = m_ref[slot, head, :] + jnp.log2(lower)

    score(0)
    for b in range(blocks):
        if b + 1 < blocks:
            score(b + 1)
        finish(b)


def attend(flags, queries, sources, pieces, swaps, guards, windows, width, before=None, later=False):
    tokens = queries.shape[0]
    rows = tokens * GROUP
    held = sum(n for _, _, n in pieces)
    wide = pl.BlockSpec((tokens, GROUP * HD), lambda h: (0, h))
    tall = pl.BlockSpec((rows, HD), lambda h: (h, 0))

    def narrow(array, offset):
        return pl.BlockSpec((array.shape[0], HD), lambda h: (0, h + offset))

    in_specs = [pl.BlockSpec(memory_space=pltpu.SMEM), wide]
    operands = [flags, queries]
    for k, k_at, v, v_at in sources:
        in_specs += [narrow(k, k_at), narrow(v, v_at)]
        operands += [k, v]
    if before is not None:
        in_specs += [wide, tall]
        operands += list(before)
    out_shape = [jax.ShapeDtypeStruct(queries.shape, jnp.bfloat16)]
    out_specs = [wide]
    if later:
        out_shape.append(jax.ShapeDtypeStruct((KVHEADS * rows, HD), jnp.float32))
        out_specs.append(tall)
    unit = GROUP * BLOCK
    return pl.pallas_call(
        functools.partial(
            attend_kernel, len(sources), pieces, swaps, guards, windows, before is not None, later
        ),
        grid=(KVHEADS,),
        in_specs=in_specs,
        out_specs=out_specs,
        out_shape=out_shape,
        scratch_shapes=[
            pltpu.VMEM((held, HD), jnp.bfloat16),
            pltpu.VMEM((held, 2 * HD), jnp.bfloat16),
            pltpu.VMEM((2, unit, width), jnp.float32),
            pltpu.VMEM((2, unit, width), jnp.bfloat16),
            pltpu.VMEM((2, unit, HD), jnp.float32),
        ],
        compiler_params=pltpu.CompilerParams(
            dimension_semantics=("arbitrary",), vmem_limit_bytes=VMEM
        ),
        cost_estimate=pl.CostEstimate(
            flops=4 * tokens * QHEADS * HD * width,
            bytes_accessed=6 * tokens * QHEADS * HD,
            transcendentals=tokens * QHEADS * width,
        ),
    )(*operands)


def placed_at(token_index):
    return (token_index % SEQ) * OUTER + token_index // SEQ


def moved(rows, source_of):
    route = [
        (placed_at(source_of(i)), placed_at(i)) for i in range(COUNT) if 0 <= source_of(i) < COUNT
    ]
    return lax.ppermute(rows, FINE, route)


def exchanged(copies, axis):
    result = lax.all_to_all(copies, axis, 0, 0, tiled=True)
    return result.reshape(-1, result.shape[-1])


def one_device(queries, keys, values):
    outer = (lax.axis_index("z_hi") * 4 + lax.axis_index("x")) * 2 + lax.axis_index("core")
    index = outer * SEQ + lax.axis_index("y") * 4 + lax.axis_index("z_lo")
    flags = [
        index > 0,
        index < COUNT - 1,
        (index >= 2) & (index < COUNT - 2),
        (outer > 0) & (outer < OUTER - 1),
        (index > 0) & (index < COUNT - 1),
        index % 2,
        (index != 1) & (index != COUNT - 2),
    ]
    flags = sum(jnp.asarray(e, jnp.int32) << k for k, e in enumerate(flags)).reshape(1)

    first, second, to_partner, to_other = pool_local(flags, keys, values)

    group = exchanged(second, ("y", "z_lo"))
    partner = moved(to_partner, lambda i: i ^ 1)
    other = moved(to_other, lambda i: i + 1 if i % 2 else i - 1)
    two = moved(first, lambda i: i ^ 2)
    third = moved(first, lambda i: i - 3 if i % 2 else i + 3)
    far = moved(first, lambda i: i - 2 if i % 4 < 2 else i + 2)

    top = exchanged(pool_again(group, 4), "z_hi")
    top = exchanged(jnp.broadcast_to(top[None], (8, *top.shape)), ("x", "core"))
    group_pair = moved(group, lambda i: i ^ SEQ)
    group_other = moved(group, lambda i: i + SEQ if (i // SEQ) % 2 else i - SEQ)

    def both(array):
        return (array, 0, array, KVHEADS)

    def whole(arrays):
        return [(k, 0, array[0].shape[0]) for k, array in enumerate(arrays)]

    rows = keys.shape[0]
    firsts = first.shape[0]
    near = [(keys, 0, values, 0)]
    near += [both(a) for a in (other, partner, first, two, third, far, group, group_pair)]
    pieces = [(1, 0, BLOCK), (0, 0, rows), (2, 0, BLOCK), (3, 0, firsts), (2, BLOCK, firsts)]
    pieces += [(1, BLOCK, firsts), (4, 0, firsts), (5, 0, firsts), (6, 0, firsts)]
    pieces += [(k, 0, BLOCK) for k in (7, 8)]
    part, lse = attend(
        flags,
        queries,
        near,
        pieces,
        [0, 2],
        {0: (0, 1), 2: (1, 1), 5: (4, 3), 7: (6, 3), 8: (2, 3)},
        lambda b: [(b * BLOCK, 3 * BLOCK), (rows + 2 * BLOCK, 5 * BLOCK)],
        8 * BLOCK,
        later=True,
    )
    coarse = [both(top), both(group_other)]
    (out,) = attend(
        flags,
        queries,
        coarse,
        whole(coarse),
        [],
        {1: (3, 0)},
        lambda b: [(0, top.shape[0] + BLOCK)],
        top.shape[0] + BLOCK,
        before=(part, lse),
    )
    return out


def solution(mesh):
    assert mesh.axis_names == ("seq", "outer")
    split = Mesh(mesh.devices.reshape(4, 4, 4, 4, 2), FINE)
    placed = P(TOKEN_ORDER, None)
    return jax.shard_map(
        one_device, mesh=split, in_specs=(placed,) * 3, out_specs=placed, check_vma=False
    )
```
